256 devices in a mesh: grp: 2 (over z), chan: 128 (over y, x, core).
Axes of the slice: x: 8, y: 8, z: 2, core: 2. Of those that a mesh axis runs over, the one named last changes fastest.
The devices are a block of a 8x8x16 slice.
Arguments:
- voltages: bfloat16 [8192, 2, 64, 128], P(('grp', 'chan')), parts along dimension 0, may hold values from -9 to 9
- delays: float32 [512, 64], replicated, may hold values from -2 to 2
- pointing: int32 [256], P('grp'), parts along dimension 0, may hold values from 0 to 511
- dm_index: int32 [256], P(('grp', 'chan')), parts along dimension 0, may hold values from 0 to 511
- dish_mask: int32 [128], P('grp'), parts along dimension 0, may hold values 0 or 1
Outputs:
- dedispersed: float32 [256, 2, 128, 4096], P(('grp', 'chan')), parts along dimension 0
The draws below stay inside these ranges and needn't reach their ends.
There are 2 independent parts, one for each index of `grp`. The reference program is written for one: setup_inputs(seed, part) draws one part's arguments, and reference() takes and returns one part's arrays. A program takes and returns all parts, laid end to end along the dimension named above; an argument that names none is the same for every part. Nothing has to cross between parts.
All inputs are finite; a program needn't handle non-finite values.
Results may differ from the reference program's by a relative error of at most 0.005.
Values may be sent and summed in bfloat16 or wider, within the bound.
A program may use at most 64 MiB of HBM per device.

```python
import math
import jax
import jax.numpy as jnp
from jax import lax

DISH = 64
CHANS = 4096
TIME = 128
LOG_LEN = 19
POINTINGS = 512
DM_TRIALS = 512
BEAMS = 128


def draw_voltages(key, part):
    base_key, rough_key = jax.random.split(key)
    array_shape = (CHANS, 2, DISH, TIME)
    channel = jnp.arange(CHANS, dtype=jnp.float32)
    roughness = jnp.exp(jax.random.uniform(rough_key, (CHANS,), minval=-0.25, maxval=0.25))
    base_draw = jnp.clip(jax.random.normal(base_key, array_shape), -4.0, 4.0)
    ramp_scale = 1.0 + 2.0 * channel / (CHANS - 1)
    chan_scale = jnp.sqrt(ramp_scale) * roughness
    return (base_draw * chan_scale[:, None, None, None]).astype(jnp.bfloat16)


def touch_ends(result, rng, low, largest):
    place = [jax.random.randint(jax.random.fold_in(rng, axis), (), 0, length) for axis, length in enumerate(result.shape)]
    widest = result.shape.index(max(result.shape))
    neighbour = place[:widest] + [(place[widest] + 1) % result.shape[widest]] + place[widest + 1:]
    return result.at[tuple(place)].set(low).at[tuple(neighbour)].set(largest)


def setup_inputs(seed: int = 0, part: int = 0) -> dict:
    key_list = jax.random.split(jax.random.key(seed), 6)
    part_splits = jax.random.split(jax.random.fold_in(key_list[5], part), 6)
    return {
        "voltages": draw_voltages(jax.random.fold_in(jax.random.fold_in(key_list[5], part), 71), part),
        "delays": jnp.clip(jax.random.uniform(key_list[1], (POINTINGS, DISH), jnp.float32, -2.0, 2.0), -2.0, 2.0),
        "pointing": touch_ends(jax.random.randint(part_splits[2], (BEAMS,), 0, POINTINGS), jax.random.fold_in(part_splits[2], 1), 0, POINTINGS - 1).astype(jnp.int32),
        "dm_index": touch_ends(jax.random.randint(part_splits[3], (BEAMS,), 0, DM_TRIALS), jax.random.fold_in(part_splits[3], 1), 0, DM_TRIALS - 1).astype(jnp.int32),
        "dish_mask": touch_ends((jax.random.randint(part_splits[4], (DISH,), 0, 8) < 7).astype(jnp.int32), jax.random.fold_in(part_splits[4], 1), 0, 1),
    }


TWO_PI = 2.0 * math.pi
BAND_LOW = 0.856
BAND_WIDTH = 0.856
EPSILON = 1e-06

def rounded(values):
    return lax.optimization_barrier(values.astype(jnp.bfloat16)).astype(jnp.float32)

def chirp_index(freq_index, rate):
    length = 2 ** LOG_LEN
    radix_len = 2 ** ((LOG_LEN + 1) // 2)
    high_part = freq_index // radix_len
    low_part = freq_index % radix_len
    squared = (2 * high_part * low_part % (length // radix_len) * radix_len + low_part * low_part) % length
    return rate * squared % length

def reference(voltages, delays, pointing, dm_index, dish_mask):
    length = TIME * CHANS
    channel = jnp.arange(CHANS, dtype=jnp.int32)
    frequency = BAND_LOW + BAND_WIDTH * (channel.astype(jnp.float32) + 0.5) / CHANS
    dish_gain = dish_mask.astype(jnp.float32) / math.sqrt(DISH)
    volt_rows = voltages.astype(jnp.float32).reshape(CHANS, 2 * DISH, TIME)
    freq_index = jnp.arange(length, dtype=jnp.int32)

    def one_beam(beam_item):
        pointing_row, trial_index = beam_item
        delay_row = delays[pointing_row]
        phase_all = (TWO_PI * frequency)[:, None] * delay_row[None, :]
        weight_re = rounded(jnp.cos(phase_all) * dish_gain)
        weight_im = rounded(-jnp.sin(phase_all) * dish_gain)
        row_re = jnp.concatenate([weight_re, -weight_im], 1)
        row_im = jnp.concatenate([weight_im, weight_re], 1)
        stacked = jnp.stack([row_re, row_im], 1)
        formed = rounded(jnp.einsum('cpk,ckt->cpt', stacked, volt_rows))
        mean_power = jnp.sum(formed * formed) / length
        channel_values = formed[:, 0] + 1j * formed[:, 1]
        chan_series = jnp.fft.ifft(channel_values, axis=0) * math.sqrt(CHANS)
        sequence = jnp.transpose(chan_series).reshape(length)
        spectrum = jnp.fft.fft(sequence)
        phase_chirp = -TWO_PI / length * chirp_index(freq_index, 2 * trial_index + 1).astype(jnp.float32)
        series = jnp.fft.ifft(spectrum * (jnp.cos(phase_chirp) + 1j * jnp.sin(phase_chirp)))
        series = series.reshape(TIME, CHANS)
        factor = lax.rsqrt(mean_power + EPSILON)
        return jnp.stack([jnp.real(series) * factor, jnp.imag(series) * factor], 0)
    return lax.map(one_beam, (pointing, dm_index))
```

```python
import functools
import math

import jax
import jax.numpy as jnp
import numpy as np
from jax import lax
from jax.experimental import pallas as pl
from jax.experimental.pallas import tpu as pltpu
from jax.sharding import PartitionSpec as P

CHANS = 4096
LOG_LEN = 19
LENGTH = 2**LOG_LEN
BAND_LOW = 0.856
BAND_WIDTH = 0.856
EPSILON = 1e-06
TWO_PI = 2.0 * math.pi
HIGHEST = lax.Precision.HIGHEST
MESH_ID = pl.DeviceIdType.MESH
VMEM_SPEC = pl.BlockSpec(memory_space=pltpu.VMEM)
SMEM_SPEC = pl.BlockSpec(memory_space=pltpu.SMEM)
ANY_SPEC = pl.BlockSpec(memory_space=pl.ANY)
LINES = 16
RADIX = 128


def circle(angle):
    square = angle * angle
    sine = angle * (
        1.0 + square * (-1.0 / 6 + square * (1.0 / 120 + square * (-1.0 / 5040 + square / 362880)))
    )
    cosine = 1.0 + square * (
        -0.5 + square * (1.0 / 24 + square * (-1.0 / 720 + square * (1.0 / 40320)))
    )
    return cosine, sine


def turned(cosine, sine, quarter):
    swap = (quarter & 1) != 0
    cos_out = jnp.where(swap, sine, cosine)
    sin_out = jnp.where(swap, cosine, sine)
    cos_out = jnp.where(((quarter + 1) & 2) != 0, -cos_out, cos_out)
    sin_out = jnp.where((quarter & 2) != 0, -sin_out, sin_out)
    return cos_out, sin_out


def circle_units(units):
    moved = units + LENGTH // 8
    quarter = (moved >> (LOG_LEN - 2)) & 3
    rest = (moved & (LENGTH // 4 - 1)) - LENGTH // 8
    cosine, sine = circle(rest.astype(jnp.float32) * (TWO_PI / LENGTH))
    return turned(cosine, sine, quarter)


def circle_turns(turns):
    quarters = jnp.floor(4.0 * turns + 0.5)
    cosine, sine = circle((turns - 0.25 * quarters) * TWO_PI)
    return turned(cosine, sine, quarters.astype(jnp.int32))


def times(a_re, a_im, b_re, b_im):
    return a_re * b_re - a_im * b_im, a_re * b_im + a_im * b_re


def four(values, sign):
    (a_re, a_im), (b_re, b_im), (c_re, c_im), (d_re, d_im) = values
    p_re, p_im = a_re + c_re, a_im + c_im
    q_re, q_im = a_re - c_re, a_im - c_im
    r_re, r_im = b_re + d_re, b_im + d_im
    t_re, t_im = b_re - d_re, b_im - d_im
    if sign > 0:
        t_re, t_im = -t_im, t_re
    else:
        t_re, t_im = t_im, -t_re
    return [
        (p_re + r_re, p_im + r_im),
        (q_re + t_re, q_im + t_im),
        (p_re - r_re, p_im - r_im),
        (q_re - t_re, q_im - t_im),
    ]


def sixteen(values, sign):
    result = [None] * 16
    inner = [four([values[4 * high + low] for high in range(4)], sign) for low in range(4)]
    for first in range(4):
        column = []
        for low in range(4):
            re_part, im_part = inner[low][first]
            power = low * first
            if power == 4:
                pair = (-im_part, re_part) if sign > 0 else (im_part, -re_part)
            elif power:
                angle = sign * TWO_PI * power / 16
                pair = times(re_part, im_part, math.cos(angle), math.sin(angle))
            else:
                pair = (re_part, im_part)
            column.append(pair)
        for second, pair in enumerate(four(column, sign)):
            result[first + 4 * second] = pair
    return result


def form_kernel(freq_ref, volt_ref, table_ref, row_ref, mask_ref, out_ref, wave, step):
    chans, rows, _ = out_ref.shape
    points = table_ref.shape[0]
    select = (
        lax.broadcasted_iota(jnp.int32, (points, rows), 0) == row_ref[...]
    ).astype(jnp.float32)
    delay = lax.dot_general(
        select, table_ref[...], (((0,), (0,)), ((), ())), precision=HIGHEST,
        preferred_element_type=jnp.float32,
    )
    delay = jnp.concatenate([delay, delay], 1)
    dishes = delay.shape[1] // 2
    part_out = lax.broadcasted_iota(jnp.int32, delay.shape, 0) & 1
    part_in = (lax.broadcasted_iota(jnp.int32, delay.shape, 1) >= dishes).astype(jnp.int32)
    offset = 0.25 * (part_in - part_out).astype(jnp.float32)
    gain = mask_ref[...].astype(jnp.float32) * (1.0 / math.sqrt(dishes))
    cosine, sine = circle_turns(freq_ref[0] * delay - offset)
    wave[0] = cosine * gain
    wave[1] = sine * gain
    cosine, sine = circle_turns((BAND_WIDTH / CHANS) * delay)
    step[0] = cosine
    step[1] = sine

    def one(chan, _):
        re_part = wave[0]
        im_part = wave[1]
        out_ref[chan] = jnp.dot(
            re_part.astype(jnp.bfloat16), volt_ref[chan], preferred_element_type=jnp.float32
        ).astype(jnp.bfloat16)
        re_next, im_next = times(re_part, im_part, step[0], step[1])
        wave[0] = re_next
        wave[1] = im_next
        return 0

    lax.fori_loop(0, chans, one, 0)


def exchange_kernel(
    sizes, rate_ref, src_ref, dst_ref, tw_ref, tm_ref, q_ref, em_ref, f_ref,
    send_sem, recv_sem,
):
    rows_y, rows_x, cores = sizes
    members = rows_y * rows_x * cores
    group = lax.axis_index("grp")
    me = lax.axis_index("chan")
    my_y = me // (rows_x * cores)
    my_x = (me // cores) % rows_x
    my_core = me % cores
    barrier = pltpu.get_barrier_semaphore()

    def greet(hop, _):
        pl.semaphore_signal(
            barrier, inc=1, device_id=(group, lax.rem(me + hop, members)),
            device_id_type=MESH_ID,
        )
        return 0

    lax.fori_loop(1, members, greet, 0)
    pl.semaphore_wait(barrier, members - 1)

    def send(hop, _):
        hop_x = (hop // cores) % rows_x
        hop_y = (hop // (cores * rows_x) + hop_x) % rows_y
        to_y = (my_y + hop_y) % rows_y
        to_x = (my_x + hop_x) % rows_x
        to = (to_y * rows_x + to_x) * cores + (my_core + hop) % cores
        pltpu.make_async_remote_copy(
            src_ref=src_ref.at[:, pl.ds(pl.multiple_of(2 * to, 2), 2)],
            dst_ref=dst_ref.at[:, pl.ds(pl.multiple_of(2 * me, 2), 2)],
            send_sem=send_sem,
            recv_sem=recv_sem,
            device_id=(group, to),
            device_id_type=MESH_ID,
        ).start()
        return 0

    lax.fori_loop(1, members, send, 0)

    rate = rate_ref[0]
    inverse = rate_ref[1]
    tables(rate, inverse, tw_ref, tm_ref, q_ref, em_ref, f_ref)

    whole = pltpu.make_async_remote_copy(
        src_ref=src_ref.at[:, pl.ds(0, 2 * (members - 1))],
        dst_ref=dst_ref.at[:, pl.ds(0, 2 * (members - 1))],
        send_sem=send_sem,
        recv_sem=recv_sem,
        device_id=(group, me),
        device_id_type=MESH_ID,
    )
    whole.wait_recv()
    whole.wait_send()
    block = pl.ds(pl.multiple_of((me // 8) * 16, 16), 16)
    shape = (src_ref.shape[0], 16, src_ref.shape[2])
    mine = lax.broadcasted_iota(jnp.int32, shape, 1) // 2 == me % 8
    dst_ref[:, block, :] = jnp.where(
        mine, src_ref[:, block, :].astype(jnp.float32), dst_ref[:, block, :].astype(jnp.float32)
    ).astype(jnp.bfloat16)


def tables(rate, inverse, tw_ref, tm_ref, q_ref, em_ref, f_ref):
    piece = 32

    def position(shape, axis):
        return lax.broadcasted_iota(jnp.int32, shape, axis)

    shape = (piece, RADIX)
    per = 2 * RADIX // piece

    def chan_turn(i, _):
        line, start = i // per, pl.multiple_of((i % per) * piece, piece)
        row = position(shape, 0) + start
        low = row & (RADIX - 1)
        chan_unit = line * (2 * low + row // RADIX) * (LENGTH // CHANS)
        cosine, sine = circle_units(
            chan_unit + inverse * (position(shape, 1) * low) * (LENGTH // RADIX)
        )
        tw_ref[0, line, pl.ds(start, piece)] = cosine
        tw_ref[1, line, pl.ds(start, piece)] = sine
        return 0

    lax.fori_loop(0, LINES * per, chan_turn, 0)

    wide = (piece, 2 * RADIX)
    per_wide = RADIX // piece

    def time_matrix(i, _):
        start = pl.multiple_of(i * piece, piece)
        time = position(wide, 0) + start
        beat = position(wide, 1) // 2
        parity = position(wide, 1) & 1
        cosine, sine = circle_units(-inverse * (time * beat) * (LENGTH // RADIX))
        for own in range(2):
            keep = parity == own
            re_part = jnp.where(keep, cosine, 0.0)
            im_part = jnp.where(keep, sine, 0.0)
            from_re = pl.ds(start + 2 * own * RADIX, piece)
            from_im = pl.ds(start + (2 * own + 1) * RADIX, piece)
            tm_ref[from_re, : 2 * RADIX] = re_part.astype(jnp.bfloat16)
            tm_ref[from_re, 2 * RADIX :] = im_part.astype(jnp.bfloat16)
            tm_ref[from_im, : 2 * RADIX] = (-im_part).astype(jnp.bfloat16)
            tm_ref[from_im, 2 * RADIX :] = re_part.astype(jnp.bfloat16)
        return 0

    lax.fori_loop(0, per_wide, time_matrix, 0)

    def wide_turn(i, _):
        line, start = i // per_wide, pl.multiple_of((i % per_wide) * piece, piece)
        low = position(wide, 0) + start
        beat = position(wide, 1) // 2
        here = pl.ds(start, piece)
        cosine, sine = circle_units(
            inverse
            * (
                low * (low - 2 * beat)
                + line * line * (LENGTH // 32)
                + line * (low - beat) * (LENGTH // 2048)
            )
        )
        q_ref[0, line, here] = cosine
        q_ref[1, line, here] = sine
        cosine, sine = circle_units(
            inverse
            * (
                beat * (beat + line * (LENGTH // 2048) + low * (LENGTH // RADIX))
                + line * line * (LENGTH // 32)
            )
            - rate * (LENGTH // 8)
        )
        f_ref[0, line, here] = cosine
        f_ref[1, line, here] = sine
        return 0

    lax.fori_loop(0, LINES * per_wide, wide_turn, 0)

    def end_matrix(i, _):
        line, start = i // per_wide, pl.multiple_of((i % per_wide) * piece, piece)
        high = position(shape, 0) + start
        cosine, sine = circle_units(
            -inverse * (position(shape, 1) * (LINES * high + line)) * (LENGTH // 2048)
        )
        upper = pl.ds(start, piece)
        lower = pl.ds(start + RADIX, piece)
        em_ref[line, upper, :RADIX] = cosine.astype(jnp.bfloat16)
        em_ref[line, upper, RADIX:] = (-sine).astype(jnp.bfloat16)
        em_ref[line, lower, :RADIX] = sine.astype(jnp.bfloat16)
        em_ref[line, lower, RADIX:] = cosine.astype(jnp.bfloat16)
        return 0

    lax.fori_loop(0, LINES * per_wide, end_matrix, 0)


def chain_kernel(
    rate_ref, x_ref, am_ref, tw_ref, tm_ref, q_ref, em_ref, f_ref, out_ref,
    grid, mid, held, total, sems,
):
    total[...] = jnp.zeros_like(total)
    for pair in range(LINES // 2):
        tops = [
            jnp.concatenate([x_ref[h * LINES + 2 * pair], x_ref[h * LINES + 2 * pair + 1]], 1)
            for h in range(2)
        ]
        data = jnp.concatenate(tops, 0)
        wide = data.astype(jnp.float32)
        total[...] += jnp.sum((wide * wide).reshape(-1, 8, 2 * RADIX), 0)
        mixed = jnp.dot(am_ref[...], data, preferred_element_type=jnp.float32)
        grid[2 * pair] = mixed[:, :RADIX]
        grid[2 * pair + 1] = mixed[:, RADIX:]

    def chan_lines(i, _):
        here = pl.ds(pl.multiple_of(i * 8, 8), 8)
        there = pl.ds(pl.multiple_of(i * 8 + 2 * RADIX, 8), 8)
        values = [
            times(grid[n, here], grid[n, there], tw_ref[0, n, here], tw_ref[1, n, here])
            for n in range(LINES)
        ]
        for n, (re_part, im_part) in enumerate(sixteen(values, 1)):
            grid[n, here] = re_part
            grid[n, there] = im_part
        return 0

    lax.fori_loop(0, 2 * RADIX // 8, chan_lines, 0)

    for quad in range(LINES // 4):
        rows = []
        for n in range(4 * quad, 4 * quad + 4):
            parts = [
                grid[n, part * 2 * RADIX + own * RADIX : part * 2 * RADIX + (own + 1) * RADIX]
                for own in range(2)
                for part in range(2)
            ]
            rows.append(jnp.concatenate(parts, 1).astype(jnp.bfloat16))
        mixed = jnp.dot(
            jnp.concatenate(rows, 0), tm_ref[...], preferred_element_type=jnp.float32
        )
        for n in range(4):
            mid[4 * quad + n] = mixed[n * RADIX : (n + 1) * RADIX]

    def beat_lines(i, _):
        here = pl.ds(pl.multiple_of(i * 8, 8), 8)
        for lane in range(0, 2 * RADIX, RADIX):
            re_at = slice(lane, lane + RADIX)
            im_at = slice(lane + 2 * RADIX, lane + 3 * RADIX)
            values = [
                times(
                    mid[n, here, re_at], mid[n, here, im_at],
                    q_ref[0, n, here, re_at], q_ref[1, n, here, re_at],
                )
                for n in range(LINES)
            ]
            for n, (re_part, im_part) in enumerate(sixteen(values, -1)):
                mid[n, here, re_at] = re_part
                mid[n, here, im_at] = im_part
        return 0

    lax.fori_loop(0, RADIX // 8, beat_lines, 0)

    power = jnp.sum(jnp.sum(total[...], 1, keepdims=True), 0, keepdims=True) * (1.0 / LENGTH)
    factor = lax.rsqrt(power + EPSILON) * (
        math.sqrt(2.0 / LENGTH) / math.sqrt(CHANS)
    )
    factor = jnp.broadcast_to(factor, (8, 2 * RADIX))[:1]
    copies = []
    for line in range(LINES):
        source = (rate_ref[1] * line) & (LINES - 1)
        data = jnp.concatenate(
            [mid[source, :, : 2 * RADIX], mid[source, :, 2 * RADIX :]], 0
        ).astype(jnp.bfloat16)
        mixed = jnp.dot(em_ref[line], data, preferred_element_type=jnp.float32)
        re_part, im_part = times(
            mixed[:RADIX], mixed[RADIX:], f_ref[0, line] * factor, f_ref[1, line] * factor
        )
        lanes = slice(line * 2 * RADIX, (line + 1) * 2 * RADIX)
        held[0, :, lanes] = re_part
        held[1, :, lanes] = im_part
        copy = pltpu.make_async_copy(
            held.at[:, :, pl.ds(line * 2 * RADIX, 2 * RADIX)],
            out_ref.at[0, :, :, pl.ds(line * 2 * RADIX, 2 * RADIX)],
            sems.at[line],
        )
        copy.start()
        copies.append(copy)
    for copy in copies:
        copy.wait()


def chan_matrix(members):
    n1 = np.arange(2 * RADIX)
    row_n1 = 2 * (n1 % RADIX) + n1 // RADIX
    half, member = np.meshgrid(np.arange(2), np.arange(members), indexing="ij")
    coarse = (2 * member + half).reshape(-1)
    angle = 2.0 * np.pi * ((row_n1[:, None] * coarse[None, :]) % (2 * RADIX)) / (2 * RADIX)
    cosine, sine = np.cos(angle), np.sin(angle)
    upper = np.stack([cosine, -sine], -1).reshape(2 * RADIX, -1)
    lower = np.stack([sine, cosine], -1).reshape(2 * RADIX, -1)
    return jnp.asarray(np.concatenate([upper, lower], 0), jnp.bfloat16)


def on_device(sizes, voltages, delays, pointing, dm_index, dish_mask):
    chan_dev, parts, dishes, samples = voltages.shape
    beams = pointing.shape[0]
    members = math.prod(sizes)
    rows = parts * beams
    first_chan = (lax.axis_index("chan") * chan_dev).astype(jnp.float32)
    frequency = (BAND_LOW + BAND_WIDTH * (first_chan + 0.5) / CHANS).reshape(1)
    rate = (2 * dm_index + 1).reshape(1)
    inverse = rate
    for _ in range(4):
        inverse = inverse * (2 - rate * inverse)
    rates = jnp.concatenate([rate, inverse & (LENGTH - 1)])
    block = jax.ShapeDtypeStruct((chan_dev, rows, samples), jnp.bfloat16)
    formed = pl.pallas_call(
        form_kernel,
        out_shape=block,
        in_specs=[SMEM_SPEC] + [VMEM_SPEC] * 4,
        out_specs=VMEM_SPEC,
        scratch_shapes=[pltpu.VMEM((2, rows, 2 * dishes), jnp.float32)] * 2,
        compiler_params=pltpu.CompilerParams(vmem_limit_bytes=12 << 20),
        name="form",
    )(
        frequency,
        voltages.reshape(chan_dev, parts * dishes, samples),
        delays,
        jnp.repeat(pointing, 2).reshape(1, rows),
        jnp.tile(dish_mask, 2).reshape(1, 2 * dishes),
    )
    wide = 2 * RADIX
    received, tw, tm, q, em, f = pl.pallas_call(
        functools.partial(exchange_kernel, sizes),
        out_shape=[
            block,
            jax.ShapeDtypeStruct((2, LINES, wide, samples), jnp.float32),
            jax.ShapeDtypeStruct((2 * wide, 2 * wide), jnp.bfloat16),
            jax.ShapeDtypeStruct((2, LINES, RADIX, wide), jnp.float32),
            jax.ShapeDtypeStruct((LINES, wide, wide), jnp.bfloat16),
            jax.ShapeDtypeStruct((2, LINES, RADIX, wide), jnp.float32),
        ],
        in_specs=[SMEM_SPEC, VMEM_SPEC],
        out_specs=[VMEM_SPEC] * 6,
        scratch_shapes=[pltpu.SemaphoreType.DMA(())] * 2,
        compiler_params=pltpu.CompilerParams(
            collective_id=0, has_side_effects=True, vmem_limit_bytes=24 << 20
        ),
        name="exchange",
    )(rates, formed)
    return pl.pallas_call(
        chain_kernel,
        out_shape=jax.ShapeDtypeStruct((1, 2, samples, CHANS), jnp.float32),
        in_specs=[SMEM_SPEC] + [VMEM_SPEC] * 7,
        out_specs=ANY_SPEC,
        scratch_shapes=[
            pltpu.VMEM((LINES, 2 * wide, samples), jnp.float32),
            pltpu.VMEM((LINES, RADIX, 2 * wide), jnp.float32),
            pltpu.VMEM((2, samples, CHANS), jnp.float32),
            pltpu.VMEM((8, wide), jnp.float32),
            pltpu.SemaphoreType.DMA((LINES,)),
        ],
        compiler_params=pltpu.CompilerParams(vmem_limit_bytes=36 << 20),
        name="chain",
    )(rates, received, chan_matrix(members), tw, tm, q, em, f)


def solution(mesh):
    members = mesh.shape["chan"]
    cores = 2
    side = math.isqrt(members // cores)
    sizes = (members // cores // side, side, cores)
    placed = (P(("grp", "chan")), P(), P("grp"), P(("grp", "chan")), P("grp"))
    return jax.shard_map(
        functools.partial(on_device, sizes),
        mesh=mesh,
        in_specs=placed,
        out_specs=P(("grp", "chan")),
        check_vma=False,
    )
```

```python
import functools
import math

import jax
import jax.numpy as jnp
import numpy as np
from jax import lax
from jax.experimental import pallas as pl
from jax.experimental.pallas import tpu as pltpu
from jax.sharding import PartitionSpec as P

CHANS = 4096
LOG_LEN = 19
LENGTH = 2**LOG_LEN
BAND_LOW = 0.856
BAND_WIDTH = 0.856
EPSILON = 1e-06
TWO_PI = 2.0 * math.pi
HIGHEST = lax.Precision.HIGHEST
MESH_ID = pl.DeviceIdType.MESH
VMEM_SPEC = pl.BlockSpec(memory_space=pltpu.VMEM)
SMEM_SPEC = pl.BlockSpec(memory_space=pltpu.SMEM)
ANY_SPEC = pl.BlockSpec(memory_space=pl.ANY)
HBM_SPEC = pl.BlockSpec(memory_space=pltpu.HBM)
LINES = 16
RADIX = 128


def circle(angle):
    square = angle * angle
    sine = angle * (
        1.0 + square * (-1.0 / 6 + square * (1.0 / 120 + square * (-1.0 / 5040 + square / 362880)))
    )
    cosine = 1.0 + square * (
        -0.5 + square * (1.0 / 24 + square * (-1.0 / 720 + square * (1.0 / 40320)))
    )
    return cosine, sine


def turned(cosine, sine, quarter):
    swap = (quarter & 1) != 0
    cos_out = jnp.where(swap, sine, cosine)
    sin_out = jnp.where(swap, cosine, sine)
    cos_out = jnp.where(((quarter + 1) & 2) != 0, -cos_out, cos_out)
    sin_out = jnp.where((quarter & 2) != 0, -sin_out, sin_out)
    return cos_out, sin_out


def circle_units(units):
    moved = units + LENGTH // 8
    quarter = (moved >> (LOG_LEN - 2)) & 3
    rest = (moved & (LENGTH // 4 - 1)) - LENGTH // 8
    cosine, sine = circle(rest.astype(jnp.float32) * (TWO_PI / LENGTH))
    return turned(cosine, sine, quarter)


def circle_turns(turns):
    quarters = jnp.floor(4.0 * turns + 0.5)
    cosine, sine = circle((turns - 0.25 * quarters) * TWO_PI)
    return turned(cosine, sine, quarters.astype(jnp.int32))


def times(a_re, a_im, b_re, b_im):
    return a_re * b_re - a_im * b_im, a_re * b_im + a_im * b_re


def four(values, sign):
    (a_re, a_im), (b_re, b_im), (c_re, c_im), (d_re, d_im) = values
    p_re, p_im = a_re + c_re, a_im + c_im
    q_re, q_im = a_re - c_re, a_im - c_im
    r_re, r_im = b_re + d_re, b_im + d_im
    t_re, t_im = b_re - d_re, b_im - d_im
    if sign > 0:
        t_re, t_im = -t_im, t_re
    else:
        t_re, t_im = t_im, -t_re
    return [
        (p_re + r_re, p_im + r_im),
        (q_re + t_re, q_im + t_im),
        (p_re - r_re, p_im - r_im),
        (q_re - t_re, q_im - t_im),
    ]


def sixteen(values, sign):
    result = [None] * 16
    inner = [four([values[4 * high + low] for high in range(4)], sign) for low in range(4)]
    for first in range(4):
        column = []
        for low in range(4):
            re_part, im_part = inner[low][first]
            power = low * first
            if power == 4:
                pair = (-im_part, re_part) if sign > 0 else (im_part, -re_part)
            elif power:
                angle = sign * TWO_PI * power / 16
                pair = times(re_part, im_part, math.cos(angle), math.sin(angle))
            else:
                pair = (re_part, im_part)
            column.append(pair)
        for second, pair in enumerate(four(column, sign)):
            result[first + 4 * second] = pair
    return result


def front_kernel(
    sizes, rate_ref, freq_ref, point_ref, mask_ref, am_ref, volt_hbm, table_hbm,
    grid_ref, total_ref, tw_ref, tm_ref, q_ref, em_ref, f_ref,
    volt, table, wave, step, formed, landed, volt_sems, table_sem, send_sem, recv_sems,
):
    rows_y, rows_x, cores = sizes
    members = rows_y * rows_x * cores
    chunks = recv_sems.shape[0]
    chunk = LINES // chunks
    slots = 2 * chunk
    group = lax.axis_index("grp")
    me = lax.axis_index("chan")
    my_y = me // (rows_x * cores)
    my_x = (me // cores) % rows_x
    my_core = me % cores

    table_copy = pltpu.make_async_copy(table_hbm, table, table_sem)
    table_copy.start()
    volt_copies = []
    for c in range(chunks):
        pair = []
        for half in range(2):
            here = pl.ds(half * LINES + c * chunk, chunk)
            copy = pltpu.make_async_copy(volt_hbm.at[here], volt.at[here], volt_sems.at[c, half])
            copy.start()
            pair.append(copy)
        volt_copies.append(pair)

    barrier = pltpu.get_barrier_semaphore()

    def greet(hop, _):
        pl.semaphore_signal(
            barrier, inc=1, device_id=(group, lax.rem(me + hop, members)),
            device_id_type=MESH_ID,
        )
        return 0

    lax.fori_loop(1, members, greet, 0)

    table_copy.wait()
    rows = formed.shape[1]
    points, beams = table.shape[1], rows // 2
    select = lax.broadcasted_iota(jnp.int32, (points, beams), 0) == point_ref[...]
    double = (
        lax.broadcasted_iota(jnp.int32, (beams, rows), 1) // 2
        == lax.broadcasted_iota(jnp.int32, (beams, rows), 0)
    )
    select = jnp.dot(
        jnp.where(select, 1.0, 0.0).astype(jnp.bfloat16),
        jnp.where(double, 1.0, 0.0).astype(jnp.bfloat16),
        preferred_element_type=jnp.float32,
    )
    delay = jnp.dot(
        table[...], select, precision=HIGHEST, preferred_element_type=jnp.float32
    )
    delay = jnp.concatenate([delay, delay], 0).T
    dishes = delay.shape[1] // 2
    part_out = lax.broadcasted_iota(jnp.int32, delay.shape, 0) & 1
    part_in = (lax.broadcasted_iota(jnp.int32, delay.shape, 1) >= dishes).astype(jnp.int32)
    offset = 0.25 * (part_in - part_out).astype(jnp.float32)
    gain = mask_ref[...].astype(jnp.float32) * (1.0 / math.sqrt(dishes))
    gain = jnp.concatenate([gain, gain], 1)
    for half in range(2):
        start = freq_ref[0] + half * LINES * BAND_WIDTH / CHANS
        cosine, sine = circle_turns(start * delay - offset)
        wave[half, 0] = cosine * gain
        wave[half, 1] = sine * gain
    cosine, sine = circle_turns((BAND_WIDTH / CHANS) * delay)
    step[0] = cosine
    step[1] = sine

    for c in range(chunks):
        for copy in volt_copies[c]:
            copy.wait()

        def form(i, _, c=c):
            for half in range(2):
                re_part = wave[half, 0]
                im_part = wave[half, 1]
                formed[c * slots + half * chunk + i] = jnp.dot(
                    re_part.astype(jnp.bfloat16),
                    volt[half * LINES + c * chunk + i],
                    preferred_element_type=jnp.float32,
                ).astype(jnp.bfloat16)
                re_next, im_next = times(re_part, im_part, step[0], step[1])
                wave[half, 0] = re_next
                wave[half, 1] = im_next
            return 0

        lax.fori_loop(0, chunk, form, 0)
        if c == 0:
            pl.semaphore_wait(barrier, members - 1)

        def send(hop, _, c=c):
            hop_x = (hop // cores) % rows_x
            hop_y = (hop // (cores * rows_x) + hop_x) % rows_y
            to_y = (my_y + hop_y) % rows_y
            to_x = (my_x + hop_x) % rows_x
            to = (to_y * rows_x + to_x) * cores + (my_core + hop) % cores
            here = pl.ds(c * slots, slots)
            pltpu.make_async_remote_copy(
                src_ref=formed.at[here, pl.ds(pl.multiple_of(2 * to, 2), 2)],
                dst_ref=landed.at[here, pl.ds(pl.multiple_of(2 * me, 2), 2)],
                send_sem=send_sem,
                recv_sem=recv_sems.at[c],
                device_id=(group, to),
                device_id_type=MESH_ID,
            ).start()
            return 0

        lax.fori_loop(1, members, send, 0)

    tables(rate_ref[0], rate_ref[1], tw_ref, tm_ref, q_ref, em_ref, f_ref)

    total_ref[...] = jnp.zeros_like(total_ref)
    block = pl.ds(pl.multiple_of((me // 8) * 16, 16), 16)
    mine = lax.broadcasted_iota(jnp.int32, (slots, 16, formed.shape[2]), 1) // 2 == me % 8
    most = pl.ds(0, 2 * (members - 1))
    for c in range(chunks):
        here = pl.ds(c * slots, slots)
        pltpu.make_async_remote_copy(
            src_ref=formed.at[here, most],
            dst_ref=landed.at[here, most],
            send_sem=send_sem,
            recv_sem=recv_sems.at[c],
            device_id=(group, me),
            device_id_type=MESH_ID,
        ).wait_recv()
        landed[here, block, :] = jnp.where(
            mine, formed[here, block, :].astype(jnp.float32),
            landed[here, block, :].astype(jnp.float32),
        ).astype(jnp.bfloat16)
        for pair in range(chunk // 2):
            first = c * slots + 2 * pair
            data = jnp.concatenate(
                [
                    jnp.concatenate(
                        [landed[first + half * chunk], landed[first + half * chunk + 1]], 1
                    )
                    for half in range(2)
                ],
                0,
            )
            wide = data.astype(jnp.float32)
            total_ref[...] += jnp.sum((wide * wide).reshape(-1, 8, 2 * RADIX), 0)
            mixed = jnp.dot(am_ref[...], data, preferred_element_type=jnp.float32)
            line = c * chunk + 2 * pair
            grid_ref[line] = mixed[:, :RADIX]
            grid_ref[line + 1] = mixed[:, RADIX:]
    pltpu.make_async_remote_copy(
        src_ref=formed.at[:, most],
        dst_ref=landed.at[:, most],
        send_sem=send_sem,
        recv_sem=recv_sems.at[0],
        device_id=(group, me),
        device_id_type=MESH_ID,
    ).wait_send()


def tables(rate, inverse, tw_ref, tm_ref, q_ref, em_ref, f_ref):
    piece = 32

    def position(shape, axis):
        return lax.broadcasted_iota(jnp.int32, shape, axis)

    shape = (piece, RADIX)
    per = 2 * RADIX // piece

    def chan_turn(i, _):
        line, start = i // per, pl.multiple_of((i % per) * piece, piece)
        row = position(shape, 0) + start
        low = row & (RADIX - 1)
        chan_unit = line * (2 * low + row // RADIX) * (LENGTH // CHANS)
        cosine, sine = circle_units(
            chan_unit + inverse * (position(shape, 1) * low) * (LENGTH // RADIX)
        )
        tw_ref[0, line, pl.ds(start, piece)] = cosine
        tw_ref[1, line, pl.ds(start, piece)] = sine
        return 0

    lax.fori_loop(0, LINES * per, chan_turn, 0)

    wide = (piece, 2 * RADIX)
    per_wide = RADIX // piece

    def time_matrix(i, _):
        start = pl.multiple_of(i * piece, piece)
        time = position(wide, 0) + start
        beat = position(wide, 1) // 2
        parity = position(wide, 1) & 1
        cosine, sine = circle_units(-inverse * (time * beat) * (LENGTH // RADIX))
        for own in range(2):
            keep = parity == own
            re_part = jnp.where(keep, cosine, 0.0)
            im_part = jnp.where(keep, sine, 0.0)
            from_re = pl.ds(start + 2 * own * RADIX, piece)
            from_im = pl.ds(start + (2 * own + 1) * RADIX, piece)
            tm_ref[from_re, : 2 * RADIX] = re_part.astype(jnp.bfloat16)
            tm_ref[from_re, 2 * RADIX :] = im_part.astype(jnp.bfloat16)
            tm_ref[from_im, : 2 * RADIX] = (-im_part).astype(jnp.bfloat16)
            tm_ref[from_im, 2 * RADIX :] = re_part.astype(jnp.bfloat16)
        return 0

    lax.fori_loop(0, per_wide, time_matrix, 0)

    def wide_turn(i, _):
        line, start = i // per_wide, pl.multiple_of((i % per_wide) * piece, piece)
        low = position(wide, 0) + start
        beat = position(wide, 1) // 2
        here = pl.ds(start, piece)
        cosine, sine = circle_units(
            inverse
            * (
                low * (low - 2 * beat)
                + line * line * (LENGTH // 32)
                + line * (low - beat) * (LENGTH // 2048)
            )
        )
        q_ref[0, line, here] = cosine
        q_ref[1, line, here] = sine
        cosine, sine = circle_units(
            inverse
            * (
                beat * (beat + line * (LENGTH // 2048) + low * (LENGTH // RADIX))
                + line * line * (LENGTH // 32)
            )
            - rate * (LENGTH // 8)
        )
        f_ref[0, line, here] = cosine
        f_ref[1, line, here] = sine
        return 0

    lax.fori_loop(0, LINES * per_wide, wide_turn, 0)

    def end_matrix(i, _):
        line, start = i // per_wide, pl.multiple_of((i % per_wide) * piece, piece)
        high = position(shape, 0) + start
        cosine, sine = circle_units(
            -inverse * (position(shape, 1) * (LINES * high + line)) * (LENGTH // 2048)
        )
        upper = pl.ds(start, piece)
        lower = pl.ds(start + RADIX, piece)
        em_ref[line, upper, :RADIX] = cosine.astype(jnp.bfloat16)
        em_ref[line, upper, RADIX:] = (-sine).astype(jnp.bfloat16)
        em_ref[line, lower, :RADIX] = sine.astype(jnp.bfloat16)
        em_ref[line, lower, RADIX:] = cosine.astype(jnp.bfloat16)
        return 0

    lax.fori_loop(0, LINES * per_wide, end_matrix, 0)


def chain_kernel(
    rate_ref, mixed_ref, total_ref, tw_ref, tm_ref, q_ref, em_ref, f_ref, out_ref,
    grid, mid, held, sems,
):
    def chan_lines(i, _):
        here = pl.ds(pl.multiple_of(i * 8, 8), 8)
        there = pl.ds(pl.multiple_of(i * 8 + 2 * RADIX, 8), 8)
        values = [
            times(mixed_ref[n, here], mixed_ref[n, there], tw_ref[0, n, here], tw_ref[1, n, here])
            for n in range(LINES)
        ]
        for n, (re_part, im_part) in enumerate(sixteen(values, 1)):
            grid[n, here] = re_part
            grid[n, there] = im_part
        return 0

    lax.fori_loop(0, 2 * RADIX // 8, chan_lines, 0)

    for quad in range(LINES // 4):
        rows = []
        for n in range(4 * quad, 4 * quad + 4):
            parts = [
                grid[n, part * 2 * RADIX + own * RADIX : part * 2 * RADIX + (own + 1) * RADIX]
                for own in range(2)
                for part in range(2)
            ]
            rows.append(jnp.concatenate(parts, 1).astype(jnp.bfloat16))
        mixed = jnp.dot(
            jnp.concatenate(rows, 0), tm_ref[...], preferred_element_type=jnp.float32
        )
        for n in range(4):
            mid[4 * quad + n] = mixed[n * RADIX : (n + 1) * RADIX]

    def beat_lines(i, _):
        here = pl.ds(pl.multiple_of(i * 8, 8), 8)
        for lane in range(0, 2 * RADIX, RADIX):
            re_at = slice(lane, lane + RADIX)
            im_at = slice(lane + 2 * RADIX, lane + 3 * RADIX)
            values = [
                times(
                    mid[n, here, re_at], mid[n, here, im_at],
                    q_ref[0, n, here, re_at], q_ref[1, n, here, re_at],
                )
                for n in range(LINES)
            ]
            for n, (re_part, im_part) in enumerate(sixteen(values, -1)):
                mid[n, here, re_at] = re_part
                mid[n, here, im_at] = im_part
        return 0

    lax.fori_loop(0, RADIX // 8, beat_lines, 0)

    power = jnp.sum(jnp.sum(total_ref[...], 1, keepdims=True), 0, keepdims=True) * (1.0 / LENGTH)
    factor = lax.rsqrt(power + EPSILON) * (
        math.sqrt(2.0 / LENGTH) / math.sqrt(CHANS)
    )
    factor = jnp.broadcast_to(factor, (8, 2 * RADIX))[:1]
    copies = []
    for line in range(LINES):
        source = (rate_ref[1] * line) & (LINES - 1)
        data = jnp.concatenate(
            [mid[source, :, : 2 * RADIX], mid[source, :, 2 * RADIX :]], 0
        ).astype(jnp.bfloat16)
        mixed = jnp.dot(em_ref[line], data, preferred_element_type=jnp.float32)
        re_part, im_part = times(
            mixed[:RADIX], mixed[RADIX:], f_ref[0, line] * factor, f_ref[1, line] * factor
        )
        lanes = slice(line * 2 * RADIX, (line + 1) * 2 * RADIX)
        held[0, :, lanes] = re_part
        held[1, :, lanes] = im_part
        copy = pltpu.make_async_copy(
            held.at[:, :, pl.ds(line * 2 * RADIX, 2 * RADIX)],
            out_ref.at[0, :, :, pl.ds(line * 2 * RADIX, 2 * RADIX)],
            sems.at[line],
        )
        copy.start()
        copies.append(copy)
    for copy in copies:
        copy.wait()


def chan_matrix(members):
    n1 = np.arange(2 * RADIX)
    row_n1 = 2 * (n1 % RADIX) + n1 // RADIX
    half, member = np.meshgrid(np.arange(2), np.arange(members), indexing="ij")
    coarse = (2 * member + half).reshape(-1)
    angle = 2.0 * np.pi * ((row_n1[:, None] * coarse[None, :]) % (2 * RADIX)) / (2 * RADIX)
    cosine, sine = np.cos(angle), np.sin(angle)
    upper = np.stack([cosine, -sine], -1).reshape(2 * RADIX, -1)
    lower = np.stack([sine, cosine], -1).reshape(2 * RADIX, -1)
    return jnp.asarray(np.concatenate([upper, lower], 0), jnp.bfloat16)


def on_device(sizes, voltages, delays, pointing, dm_index, dish_mask):
    chan_dev, parts, dishes, samples = voltages.shape
    beams = pointing.shape[0]
    members = math.prod(sizes)
    rows = parts * beams
    first_chan = (lax.axis_index("chan") * chan_dev).astype(jnp.float32)
    frequency = (BAND_LOW + BAND_WIDTH * (first_chan + 0.5) / CHANS).reshape(1)
    rate = (2 * dm_index + 1).reshape(1)
    inverse = rate
    for _ in range(4):
        inverse = inverse * (2 - rate * inverse)
    rates = jnp.concatenate([rate, inverse & (LENGTH - 1)])
    wide = 2 * RADIX
    chunks = 4
    mixed, total, tw, tm, q, em, f = pl.pallas_call(
        functools.partial(front_kernel, sizes),
        out_shape=[
            jax.ShapeDtypeStruct((LINES, 2 * wide, samples), jnp.float32),
            jax.ShapeDtypeStruct((8, wide), jnp.float32),
            jax.ShapeDtypeStruct((2, LINES, wide, samples), jnp.float32),
            jax.ShapeDtypeStruct((2 * wide, 2 * wide), jnp.bfloat16),
            jax.ShapeDtypeStruct((2, LINES, RADIX, wide), jnp.float32),
            jax.ShapeDtypeStruct((LINES, wide, wide), jnp.bfloat16),
            jax.ShapeDtypeStruct((2, LINES, RADIX, wide), jnp.float32),
        ],
        in_specs=[SMEM_SPEC] * 2 + [VMEM_SPEC] * 3 + [HBM_SPEC] * 2,
        out_specs=[VMEM_SPEC] * 7,
        scratch_shapes=[
            pltpu.VMEM((chan_dev, parts * dishes, samples), jnp.bfloat16),
            pltpu.VMEM(delays.shape[::-1], jnp.float32),
            pltpu.VMEM((2, 2, rows, parts * dishes), jnp.float32),
            pltpu.VMEM((2, rows, parts * dishes), jnp.float32),
            pltpu.VMEM((chan_dev, rows, samples), jnp.bfloat16),
            pltpu.VMEM((chan_dev, rows, samples), jnp.bfloat16),
            pltpu.SemaphoreType.DMA((chunks, 2)),
            pltpu.SemaphoreType.DMA(()),
            pltpu.SemaphoreType.DMA(()),
            pltpu.SemaphoreType.DMA((chunks,)),
        ],
        compiler_params=pltpu.CompilerParams(
            collective_id=0, has_side_effects=True, vmem_limit_bytes=20 << 20
        ),
        name="front",
    )(
        rates,
        frequency,
        pointing.reshape(1, beams),
        dish_mask.reshape(1, dishes),
        chan_matrix(members),
        pltpu.with_memory_space_constraint(
            voltages.reshape(chan_dev, parts * dishes, samples), pltpu.HBM
        ),
        pltpu.with_memory_space_constraint(delays.T, pltpu.HBM),
    )
    return pl.pallas_call(
        chain_kernel,
        out_shape=jax.ShapeDtypeStruct((1, 2, samples, CHANS), jnp.float32),
        in_specs=[SMEM_SPEC] + [VMEM_SPEC] * 7,
        out_specs=ANY_SPEC,
        scratch_shapes=[
            pltpu.VMEM((LINES, 2 * wide, samples), jnp.float32),
            pltpu.VMEM((LINES, RADIX, 2 * wide), jnp.float32),
            pltpu.VMEM((2, samples, CHANS), jnp.float32),
            pltpu.SemaphoreType.DMA((LINES,)),
        ],
        compiler_params=pltpu.CompilerParams(vmem_limit_bytes=20 << 20),
        name="chain",
    )(rates, mixed, total, tw, tm, q, em, f)


def solution(mesh):
    members = mesh.shape["chan"]
    cores = 2
    side = math.isqrt(members // cores)
    sizes = (members // cores // side, side, cores)
    placed = (P(("grp", "chan")), P(), P("grp"), P(("grp", "chan")), P("grp"))
    return jax.shard_map(
        functools.partial(on_device, sizes),
        mesh=mesh,
        in_specs=placed,
        out_specs=P(("grp", "chan")),
        check_vma=False,
    )
```

```python
import functools
import math

import jax
import jax.numpy as jnp
import numpy as np
from jax import lax
from jax.experimental import pallas as pl
from jax.experimental.pallas import tpu as pltpu
from jax.sharding import PartitionSpec as P

CHANS = 4096
LOG_LEN = 19
LENGTH = 2**LOG_LEN
BAND_LOW = 0.856
BAND_WIDTH = 0.856
EPSILON = 1e-06
TWO_PI = 2.0 * math.pi
HIGHEST = lax.Precision.HIGHEST
MESH_ID = pl.DeviceIdType.MESH
VMEM_SPEC = pl.BlockSpec(memory_space=pltpu.VMEM)
SMEM_SPEC = pl.BlockSpec(memory_space=pltpu.SMEM)
ANY_SPEC = pl.BlockSpec(memory_space=pl.ANY)
HBM_SPEC = pl.BlockSpec(memory_space=pltpu.HBM)
LINES = 16
RADIX = 128
SPREAD = 45


def circle(angle):
    square = angle * angle
    sine = angle * (
        1.0 + square * (-1.0 / 6 + square * (1.0 / 120 + square * (-1.0 / 5040 + square / 362880)))
    )
    cosine = 1.0 + square * (
        -0.5 + square * (1.0 / 24 + square * (-1.0 / 720 + square * (1.0 / 40320)))
    )
    return cosine, sine


def turned(cosine, sine, quarter):
    swap = (quarter & 1) != 0
    cos_out = jnp.where(swap, sine, cosine)
    sin_out = jnp.where(swap, cosine, sine)
    cos_out = jnp.where(((quarter + 1) & 2) != 0, -cos_out, cos_out)
    sin_out = jnp.where((quarter & 2) != 0, -sin_out, sin_out)
    return cos_out, sin_out


def circle_units(units):
    moved = units + LENGTH // 8
    quarter = (moved >> (LOG_LEN - 2)) & 3
    rest = (moved & (LENGTH // 4 - 1)) - LENGTH // 8
    cosine, sine = circle(rest.astype(jnp.float32) * (TWO_PI / LENGTH))
    return turned(cosine, sine, quarter)


def circle_turns(turns):
    quarters = jnp.floor(4.0 * turns + 0.5)
    cosine, sine = circle((turns - 0.25 * quarters) * TWO_PI)
    return turned(cosine, sine, quarters.astype(jnp.int32))


def times(a_re, a_im, b_re, b_im):
    return a_re * b_re - a_im * b_im, a_re * b_im + a_im * b_re


def four(values, sign):
    (a_re, a_im), (b_re, b_im), (c_re, c_im), (d_re, d_im) = values
    p_re, p_im = a_re + c_re, a_im + c_im
    q_re, q_im = a_re - c_re, a_im - c_im
    r_re, r_im = b_re + d_re, b_im + d_im
    t_re, t_im = b_re - d_re, b_im - d_im
    if sign > 0:
        t_re, t_im = -t_im, t_re
    else:
        t_re, t_im = t_im, -t_re
    return [
        (p_re + r_re, p_im + r_im),
        (q_re + t_re, q_im + t_im),
        (p_re - r_re, p_im - r_im),
        (q_re - t_re, q_im - t_im),
    ]


def sixteenth(pair, power, sign):
    re_part, im_part = pair
    if power == 0:
        return pair
    if power == 4:
        return (-im_part, re_part) if sign > 0 else (im_part, -re_part)
    angle = sign * TWO_PI * power / 16
    return times(re_part, im_part, math.cos(angle), math.sin(angle))


def sixteen(values, sign):
    result = [None] * 16
    inner = [four([values[4 * high + low] for high in range(4)], sign) for low in range(4)]
    for first in range(4):
        column = []
        for low in range(4):
            column.append(sixteenth(inner[low][first], low * first, sign))
        for second, pair in enumerate(four(column, sign)):
            result[first + 4 * second] = pair
    return result


def front_kernel(
    sizes, rate_ref, freq_ref, point_hbm, mask_hbm, am_hbm, volt_hbm, table_hbm,
    grid_ref, total_ref, tw_ref, tm_ref, q_ref, em_ref, f_ref,
    volt, table, point_ref, mask_ref, am_ref, wave, step, formed, landed,
    volt_sems, small_sems, send_sem, recv_sems,
):
    rows_y, rows_x, cores = sizes
    members = rows_y * rows_x * cores
    chunks = recv_sems.shape[0]
    chunk = LINES // chunks
    slots = 2 * chunk
    group = lax.axis_index("grp")
    me = lax.axis_index("chan")
    my_y = me // (rows_x * cores)
    my_x = (me // cores) % rows_x
    my_core = me % cores

    small_copies = [
        pltpu.make_async_copy(point_hbm, point_ref, small_sems.at[0]),
        pltpu.make_async_copy(table_hbm, table, small_sems.at[1]),
        pltpu.make_async_copy(mask_hbm, mask_ref, small_sems.at[2]),
        pltpu.make_async_copy(am_hbm, am_ref, small_sems.at[3]),
    ]
    volt_copies = [
        pltpu.make_async_copy(volt_hbm.at[:, c], volt.at[:, c], volt_sems.at[c])
        for c in range(chunks)
    ]
    for copy in small_copies[:3] + volt_copies + small_copies[3:]:
        copy.start()

    barrier = pltpu.get_barrier_semaphore()

    def greet(hop, _):
        pl.semaphore_signal(
            barrier, inc=1, device_id=(group, lax.rem(me + hop, members)),
            device_id_type=MESH_ID,
        )
        return 0

    lax.fori_loop(1, members, greet, 0)

    for copy in small_copies[:3]:
        copy.wait()
    rows = formed.shape[1]
    points, beams = table.shape[1], rows // 2
    select = lax.broadcasted_iota(jnp.int32, (points, beams), 0) == point_ref[...]
    double = (
        lax.broadcasted_iota(jnp.int32, (beams, rows), 1) // 2
        == lax.broadcasted_iota(jnp.int32, (beams, rows), 0)
    )
    select = jnp.dot(
        jnp.where(select, 1.0, 0.0).astype(jnp.bfloat16),
        jnp.where(double, 1.0, 0.0).astype(jnp.bfloat16),
        preferred_element_type=jnp.float32,
    )
    delay = jnp.dot(
        table[...], select, precision=HIGHEST, preferred_element_type=jnp.float32
    )
    delay = jnp.concatenate([delay, delay], 0).T
    dishes = delay.shape[1] // 2
    part_out = lax.broadcasted_iota(jnp.int32, delay.shape, 0) & 1
    part_in = (lax.broadcasted_iota(jnp.int32, delay.shape, 1) >= dishes).astype(jnp.int32)
    offset = 0.25 * (part_in - part_out).astype(jnp.float32)
    gain = mask_ref[...].astype(jnp.float32) * (1.0 / math.sqrt(dishes))
    gain = jnp.concatenate([gain, gain], 1)
    def turn(chans):
        return circle_turns((chans * BAND_WIDTH / CHANS) * delay)

    cosine, sine = circle_turns(freq_ref[0] * delay - offset)
    wave[0, 0] = cosine * gain
    wave[0, 1] = sine * gain
    step[0], step[1] = turn(chunks)
    for slot in range(1, chunk):
        wave[slot, 0], wave[slot, 1] = times(
            wave[slot - 1, 0], wave[slot - 1, 1], step[0], step[1]
        )
    step[0], step[1] = turn(LINES)
    for slot in range(chunk, slots):
        wave[slot, 0], wave[slot, 1] = times(
            wave[slot - chunk, 0], wave[slot - chunk, 1], step[0], step[1]
        )
    step[0], step[1] = turn(1)

    for c in range(chunks):
        volt_copies[c].wait()

        def form(slot, _, c=c):
            re_part = wave[slot, 0]
            im_part = wave[slot, 1]
            formed[c * slots + slot] = jnp.dot(
                re_part.astype(jnp.bfloat16), volt[slot, c], preferred_element_type=jnp.float32
            ).astype(jnp.bfloat16)
            wave[slot, 0], wave[slot, 1] = times(re_part, im_part, step[0], step[1])
            return 0

        lax.fori_loop(0, slots, form, 0)
        if c == 0:
            pl.semaphore_wait(barrier, members - 1)

        def send(hop, _, c=c):
            place = (hop * SPREAD) % members
            hop_x = (place // cores) % rows_x
            hop_y = place // (cores * rows_x)
            to_y = (my_y + rows_y + hop_y * (1 - 2 * my_core)) % rows_y
            to_x = (my_x + rows_x + hop_x * (1 - 2 * my_core)) % rows_x
            to = (to_y * rows_x + to_x) * cores + (my_core + place) % cores
            here = pl.ds(c * slots, slots)
            pltpu.make_async_remote_copy(
                src_ref=formed.at[here, pl.ds(pl.multiple_of(2 * to, 2), 2)],
                dst_ref=landed.at[here, pl.ds(pl.multiple_of(2 * me, 2), 2)],
                send_sem=send_sem,
                recv_sem=recv_sems.at[c],
                device_id=(group, to),
                device_id_type=MESH_ID,
            ).start()
            return 0

        lax.fori_loop(1, members, send, 0)

    small_copies[3].wait()
    tables(rate_ref[0], rate_ref[1], tw_ref, tm_ref, q_ref, em_ref, f_ref)

    total_ref[...] = jnp.zeros_like(total_ref)
    block = pl.ds(pl.multiple_of((me // 8) * 16, 16), 16)
    mine = lax.broadcasted_iota(jnp.int32, (slots, 16, formed.shape[2]), 1) // 2 == me % 8
    most = pl.ds(0, 2 * (members - 1))
    for c in range(chunks):
        here = pl.ds(c * slots, slots)
        pltpu.make_async_remote_copy(
            src_ref=formed.at[here, most],
            dst_ref=landed.at[here, most],
            send_sem=send_sem,
            recv_sem=recv_sems.at[c],
            device_id=(group, me),
            device_id_type=MESH_ID,
        ).wait_recv()
        landed[here, block, :] = jnp.where(
            mine, formed[here, block, :].astype(jnp.float32),
            landed[here, block, :].astype(jnp.float32),
        ).astype(jnp.bfloat16)
        for pair in range(chunk // 2):
            first = c * slots + 2 * pair
            data = jnp.concatenate(
                [
                    jnp.concatenate(
                        [landed[first + half * chunk], landed[first + half * chunk + 1]], 1
                    )
                    for half in range(2)
                ],
                0,
            )
            wide = data.astype(jnp.float32)
            total_ref[...] += jnp.sum((wide * wide).reshape(-1, 8, 2 * RADIX), 0)
            mixed = jnp.dot(am_ref[...], data, preferred_element_type=jnp.float32)
            grid_ref[c + 2 * pair * chunks] = mixed[:, :RADIX]
            grid_ref[c + (2 * pair + 1) * chunks] = mixed[:, RADIX:]

        def chan_fours(i, _, c=c):
            here = pl.ds(pl.multiple_of(i * 16, 16), 16)
            there = pl.ds(pl.multiple_of(i * 16 + 2 * RADIX, 16), 16)
            lines = [c + chunks * high for high in range(4)]
            values = [
                times(grid_ref[n, here], grid_ref[n, there], tw_ref[0, n, here], tw_ref[1, n, here])
                for n in lines
            ]
            for first, pair in enumerate(four(values, 1)):
                re_part, im_part = sixteenth(pair, c * first, 1)
                grid_ref[lines[first], here] = re_part
                grid_ref[lines[first], there] = im_part
            return 0

        lax.fori_loop(0, 2 * RADIX // 16, chan_fours, 0)
    pltpu.make_async_remote_copy(
        src_ref=formed.at[:, most],
        dst_ref=landed.at[:, most],
        send_sem=send_sem,
        recv_sem=recv_sems.at[0],
        device_id=(group, me),
        device_id_type=MESH_ID,
    ).wait_send()


def tables(rate, inverse, tw_ref, tm_ref, q_ref, em_ref, f_ref):
    piece = 32

    def position(shape, axis):
        return lax.broadcasted_iota(jnp.int32, shape, axis)

    shape = (piece, RADIX)
    per = 2 * RADIX // piece

    def chan_turn(i, _):
        line, start = i // per, pl.multiple_of((i % per) * piece, piece)
        row = position(shape, 0) + start
        low = row & (RADIX - 1)
        chan_unit = line * (2 * low + row // RADIX) * (LENGTH // CHANS)
        cosine, sine = circle_units(
            chan_unit + inverse * (position(shape, 1) * low) * (LENGTH // RADIX)
        )
        tw_ref[0, line, pl.ds(start, piece)] = cosine
        tw_ref[1, line, pl.ds(start, piece)] = sine
        return 0

    lax.fori_loop(0, LINES * per, chan_turn, 0)

    wide = (piece, 2 * RADIX)
    per_wide = RADIX // piece

    def time_matrix(i, _):
        start = pl.multiple_of(i * piece, piece)
        time = position(wide, 0) + start
        beat = position(wide, 1) // 2
        parity = position(wide, 1) & 1
        cosine, sine = circle_units(-inverse * (time * beat) * (LENGTH // RADIX))
        for own in range(2):
            keep = parity == own
            re_part = jnp.where(keep, cosine, 0.0)
            im_part = jnp.where(keep, sine, 0.0)
            from_re = pl.ds(start + 2 * own * RADIX, piece)
            from_im = pl.ds(start + (2 * own + 1) * RADIX, piece)
            tm_ref[from_re, : 2 * RADIX] = re_part.astype(jnp.bfloat16)
            tm_ref[from_re, 2 * RADIX :] = im_part.astype(jnp.bfloat16)
            tm_ref[from_im, : 2 * RADIX] = (-im_part).astype(jnp.bfloat16)
            tm_ref[from_im, 2 * RADIX :] = re_part.astype(jnp.bfloat16)
        return 0

    lax.fori_loop(0, per_wide, time_matrix, 0)

    def wide_turn(i, _):
        line, start = i // per_wide, pl.multiple_of((i % per_wide) * piece, piece)
        low = position(wide, 0) + start
        beat = position(wide, 1) // 2
        here = pl.ds(start, piece)
        cosine, sine = circle_units(
            inverse
            * (
                low * (low - 2 * beat)
                + line * line * (LENGTH // 32)
                + line * (low - beat) * (LENGTH // 2048)
            )
        )
        q_ref[0, line, here] = cosine
        q_ref[1, line, here] = sine
        cosine, sine = circle_units(
            inverse
            * (
                beat * (beat + line * (LENGTH // 2048) + low * (LENGTH // RADIX))
                + line * line * (LENGTH // 32)
            )
            - rate * (LENGTH // 8)
        )
        f_ref[0, line, here] = cosine
        f_ref[1, line, here] = sine
        return 0

    lax.fori_loop(0, LINES * per_wide, wide_turn, 0)

    def end_matrix(i, _):
        line, start = i // per_wide, pl.multiple_of((i % per_wide) * piece, piece)
        high = position(shape, 0) + start
        cosine, sine = circle_units(
            -inverse * (position(shape, 1) * (LINES * high + line)) * (LENGTH // 2048)
        )
        upper = pl.ds(start, piece)
        lower = pl.ds(start + RADIX, piece)
        em_ref[line, upper, :RADIX] = cosine.astype(jnp.bfloat16)
        em_ref[line, upper, RADIX:] = (-sine).astype(jnp.bfloat16)
        em_ref[line, lower, :RADIX] = sine.astype(jnp.bfloat16)
        em_ref[line, lower, RADIX:] = cosine.astype(jnp.bfloat16)
        return 0

    lax.fori_loop(0, LINES * per_wide, end_matrix, 0)


def chain_kernel(
    rate_ref, mixed_ref, total_ref, tw_ref, tm_ref, q_ref, em_ref, f_ref, out_ref,
    grid, mid, held, sems,
):
    def chan_lines(i, _):
        here = pl.ds(pl.multiple_of(i * 8, 8), 8)
        there = pl.ds(pl.multiple_of(i * 8 + 2 * RADIX, 8), 8)
        for first in range(4):
            column = [
                (mixed_ref[low + 4 * first, here], mixed_ref[low + 4 * first, there])
                for low in range(4)
            ]
            for second, (re_part, im_part) in enumerate(four(column, 1)):
                grid[first + 4 * second, here] = re_part
                grid[first + 4 * second, there] = im_part
        return 0

    lax.fori_loop(0, 2 * RADIX // 8, chan_lines, 0)

    for quad in range(LINES // 4):
        rows = []
        for n in range(4 * quad, 4 * quad + 4):
            parts = [
                grid[n, part * 2 * RADIX + own * RADIX : part * 2 * RADIX + (own + 1) * RADIX]
                for own in range(2)
                for part in range(2)
            ]
            rows.append(jnp.concatenate(parts, 1).astype(jnp.bfloat16))
        mixed = jnp.dot(
            jnp.concatenate(rows, 0), tm_ref[...], preferred_element_type=jnp.float32
        )
        for n in range(4):
            mid[4 * quad + n] = mixed[n * RADIX : (n + 1) * RADIX]

    def beat_lines(i, _):
        here = pl.ds(pl.multiple_of(i * 8, 8), 8)
        for lane in range(0, 2 * RADIX, RADIX):
            re_at = slice(lane, lane + RADIX)
            im_at = slice(lane + 2 * RADIX, lane + 3 * RADIX)
            values = [
                times(
                    mid[n, here, re_at], mid[n, here, im_at],
                    q_ref[0, n, here, re_at], q_ref[1, n, here, re_at],
                )
                for n in range(LINES)
            ]
            for n, (re_part, im_part) in enumerate(sixteen(values, -1)):
                mid[n, here, re_at] = re_part
                mid[n, here, im_at] = im_part
        return 0

    lax.fori_loop(0, RADIX // 8, beat_lines, 0)

    power = jnp.sum(jnp.sum(total_ref[...], 1, keepdims=True), 0, keepdims=True) * (1.0 / LENGTH)
    factor = lax.rsqrt(power + EPSILON) * (
        math.sqrt(2.0 / LENGTH) / math.sqrt(CHANS)
    )
    factor = jnp.broadcast_to(factor, (8, 2 * RADIX))[:1]
    copies = []
    for line in range(LINES):
        source = (rate_ref[1] * line) & (LINES - 1)
        data = jnp.concatenate(
            [mid[source, :, : 2 * RADIX], mid[source, :, 2 * RADIX :]], 0
        ).astype(jnp.bfloat16)
        mixed = jnp.dot(em_ref[line], data, preferred_element_type=jnp.float32)
        re_part, im_part = times(
            mixed[:RADIX], mixed[RADIX:], f_ref[0, line] * factor, f_ref[1, line] * factor
        )
        lanes = slice(line * 2 * RADIX, (line + 1) * 2 * RADIX)
        held[0, :, lanes] = re_part
        held[1, :, lanes] = im_part
        copy = pltpu.make_async_copy(
            held.at[:, :, pl.ds(line * 2 * RADIX, 2 * RADIX)],
            out_ref.at[0, :, :, pl.ds(line * 2 * RADIX, 2 * RADIX)],
            sems.at[line],
        )
        copy.start()
        copies.append(copy)
    for copy in copies:
        copy.wait()


def chan_matrix(members):
    n1 = np.arange(2 * RADIX)
    row_n1 = 2 * (n1 % RADIX) + n1 // RADIX
    half, member = np.meshgrid(np.arange(2), np.arange(members), indexing="ij")
    coarse = (2 * member + half).reshape(-1)
    angle = 2.0 * np.pi * ((row_n1[:, None] * coarse[None, :]) % (2 * RADIX)) / (2 * RADIX)
    cosine, sine = np.cos(angle), np.sin(angle)
    upper = np.stack([cosine, -sine], -1).reshape(2 * RADIX, -1)
    lower = np.stack([sine, cosine], -1).reshape(2 * RADIX, -1)
    return jnp.asarray(np.concatenate([upper, lower], 0), jnp.bfloat16)


def on_device(sizes, voltages, delays, pointing, dm_index, dish_mask):
    chan_dev, parts, dishes, samples = voltages.shape
    beams = pointing.shape[0]
    members = math.prod(sizes)
    rows = parts * beams
    first_chan = (lax.axis_index("chan") * chan_dev).astype(jnp.float32)
    frequency = (BAND_LOW + BAND_WIDTH * (first_chan + 0.5) / CHANS).reshape(1)
    rate = (2 * dm_index + 1).reshape(1)
    inverse = rate
    for _ in range(4):
        inverse = inverse * (2 - rate * inverse)
    rates = jnp.concatenate([rate, inverse & (LENGTH - 1)])
    wide = 2 * RADIX
    chunks = 4
    slots = chan_dev // chunks
    mixed, total, tw, tm, q, em, f = pl.pallas_call(
        functools.partial(front_kernel, sizes),
        out_shape=[
            jax.ShapeDtypeStruct((LINES, 2 * wide, samples), jnp.float32),
            jax.ShapeDtypeStruct((8, wide), jnp.float32),
            jax.ShapeDtypeStruct((2, LINES, wide, samples), jnp.float32),
            jax.ShapeDtypeStruct((2 * wide, 2 * wide), jnp.bfloat16),
            jax.ShapeDtypeStruct((2, LINES, RADIX, wide), jnp.float32),
            jax.ShapeDtypeStruct((LINES, wide, wide), jnp.bfloat16),
            jax.ShapeDtypeStruct((2, LINES, RADIX, wide), jnp.float32),
        ],
        in_specs=[SMEM_SPEC] * 2 + [HBM_SPEC] * 5,
        out_specs=[VMEM_SPEC] * 7,
        scratch_shapes=[
            pltpu.VMEM((slots, chunks, parts * dishes, samples), jnp.bfloat16),
            pltpu.VMEM(delays.shape[::-1], jnp.float32),
            pltpu.VMEM((1, beams), jnp.int32),
            pltpu.VMEM((1, dishes), jnp.int32),
            pltpu.VMEM((2 * wide, 2 * wide), jnp.bfloat16),
            pltpu.VMEM((slots, 2, rows, parts * dishes), jnp.float32),
            pltpu.VMEM((2, rows, parts * dishes), jnp.float32),
            pltpu.VMEM((chan_dev, rows, samples), jnp.bfloat16),
            pltpu.VMEM((chan_dev, rows, samples), jnp.bfloat16),
            pltpu.SemaphoreType.DMA((chunks,)),
            pltpu.SemaphoreType.DMA((4,)),
            pltpu.SemaphoreType.DMA(()),
            pltpu.SemaphoreType.DMA((chunks,)),
        ],
        compiler_params=pltpu.CompilerParams(
            collective_id=0, has_side_effects=True, vmem_limit_bytes=20 << 20
        ),
        name="front",
    )(
        rates,
        frequency,
        *(
            pltpu.with_memory_space_constraint(value, pltpu.HBM)
            for value in (
                pointing.reshape(1, beams),
                dish_mask.reshape(1, dishes),
                chan_matrix(members),
                voltages.reshape(slots, chunks, parts * dishes, samples),
                delays.T,
            )
        ),
    )
    return pl.pallas_call(
        chain_kernel,
        out_shape=jax.ShapeDtypeStruct((1, 2, samples, CHANS), jnp.float32),
        in_specs=[SMEM_SPEC] + [VMEM_SPEC] * 7,
        out_specs=ANY_SPEC,
        scratch_shapes=[
            pltpu.VMEM((LINES, 2 * wide, samples), jnp.float32),
            pltpu.VMEM((LINES, RADIX, 2 * wide), jnp.float32),
            pltpu.VMEM((2, samples, CHANS), jnp.float32),
            pltpu.SemaphoreType.DMA((LINES,)),
        ],
        compiler_params=pltpu.CompilerParams(vmem_limit_bytes=20 << 20),
        name="chain",
    )(rates, mixed, total, tw, tm, q, em, f)


def solution(mesh):
    members = mesh.shape["chan"]
    cores = 2
    side = math.isqrt(members // cores)
    sizes = (members // cores // side, side, cores)
    placed = (P(("grp", "chan")), P(), P("grp"), P(("grp", "chan")), P("grp"))
    return jax.shard_map(
        functools.partial(on_device, sizes),
        mesh=mesh,
        in_specs=placed,
        out_specs=P(("grp", "chan")),
        check_vma=False,
    )
```

```python
import functools
import math

import jax
import jax.numpy as jnp
import numpy as np
from jax import lax
from jax.experimental import pallas as pl
from jax.experimental.pallas import tpu as pltpu
from jax.sharding import PartitionSpec as P

CHANS = 4096
LOG_LEN = 19
LENGTH = 2**LOG_LEN
BAND_LOW = 0.856
BAND_WIDTH = 0.856
EPSILON = 1e-06
TWO_PI = 2.0 * math.pi
HIGHEST = lax.Precision.HIGHEST
MESH_ID = pl.DeviceIdType.MESH
VMEM_SPEC = pl.BlockSpec(memory_space=pltpu.VMEM)
SMEM_SPEC = pl.BlockSpec(memory_space=pltpu.SMEM)
ANY_SPEC = pl.BlockSpec(memory_space=pl.ANY)
HBM_SPEC = pl.BlockSpec(memory_space=pltpu.HBM)
LINES = 16
RADIX = 128
GROUPED = 7
SPREAD = 45


def circle(angle):
    square = angle * angle
    sine = angle * (
        1.0 + square * (-1.0 / 6 + square * (1.0 / 120 + square * (-1.0 / 5040 + square / 362880)))
    )
    cosine = 1.0 + square * (
        -0.5 + square * (1.0 / 24 + square * (-1.0 / 720 + square * (1.0 / 40320)))
    )
    return cosine, sine


def turned(cosine, sine, quarter):
    swap = (quarter & 1) != 0
    cos_out = jnp.where(swap, sine, cosine)
    sin_out = jnp.where(swap, cosine, sine)
    cos_out = jnp.where(((quarter + 1) & 2) != 0, -cos_out, cos_out)
    sin_out = jnp.where((quarter & 2) != 0, -sin_out, sin_out)
    return cos_out, sin_out


def circle_units(units):
    moved = units + LENGTH // 8
    quarter = (moved >> (LOG_LEN - 2)) & 3
    rest = (moved & (LENGTH // 4 - 1)) - LENGTH // 8
    cosine, sine = circle(rest.astype(jnp.float32) * (TWO_PI / LENGTH))
    return turned(cosine, sine, quarter)


def circle_turns(turns):
    quarters = jnp.floor(4.0 * turns + 0.5)
    cosine, sine = circle((turns - 0.25 * quarters) * TWO_PI)
    return turned(cosine, sine, quarters.astype(jnp.int32))


def times(a_re, a_im, b_re, b_im):
    return a_re * b_re - a_im * b_im, a_re * b_im + a_im * b_re


def four(values, sign):
    (a_re, a_im), (b_re, b_im), (c_re, c_im), (d_re, d_im) = values
    p_re, p_im = a_re + c_re, a_im + c_im
    q_re, q_im = a_re - c_re, a_im - c_im
    r_re, r_im = b_re + d_re, b_im + d_im
    t_re, t_im = b_re - d_re, b_im - d_im
    if sign > 0:
        t_re, t_im = -t_im, t_re
    else:
        t_re, t_im = t_im, -t_re
    return [
        (p_re + r_re, p_im + r_im),
        (q_re + t_re, q_im + t_im),
        (p_re - r_re, p_im - r_im),
        (q_re - t_re, q_im - t_im),
    ]


def sixteenth(pair, power, sign):
    re_part, im_part = pair
    if power == 0:
        return pair
    if power == 4:
        return (-im_part, re_part) if sign > 0 else (im_part, -re_part)
    angle = sign * TWO_PI * power / 16
    return times(re_part, im_part, math.cos(angle), math.sin(angle))


def sixteen(values, sign):
    result = [None] * 16
    inner = [four([values[4 * high + low] for high in range(4)], sign) for low in range(4)]
    for first in range(4):
        column = []
        for low in range(4):
            column.append(sixteenth(inner[low][first], low * first, sign))
        for second, pair in enumerate(four(column, sign)):
            result[first + 4 * second] = pair
    return result


def front_kernel(
    sizes, rate_ref, freq_ref, point_hbm, mask_hbm, am_hbm, volt_hbm, table_hbm,
    grid_ref, total_ref, tw_ref, tm_ref, q_ref, em_ref, f_ref,
    volt, table, point_ref, mask_ref, am_ref, wave, step, formed, landed,
    volt_sems, small_sems, send_sem, recv_sems,
):
    rows_y, rows_x, cores = sizes
    chips = rows_y * rows_x
    members = chips * cores
    chunks = recv_sems.shape[0]
    chunk = LINES // chunks
    slots = 2 * chunk
    group = lax.axis_index("grp")
    me = lax.axis_index("chan")
    my_y = me // (rows_x * cores)
    my_x = (me // cores) % rows_x
    my_core = me % cores

    small_copies = [
        pltpu.make_async_copy(point_hbm, point_ref, small_sems.at[0]),
        pltpu.make_async_copy(table_hbm, table, small_sems.at[1]),
        pltpu.make_async_copy(mask_hbm, mask_ref, small_sems.at[2]),
        pltpu.make_async_copy(am_hbm, am_ref, small_sems.at[3]),
    ]
    volt_copies = [
        pltpu.make_async_copy(volt_hbm.at[:, c], volt.at[:, c], volt_sems.at[c])
        for c in range(chunks)
    ]
    for copy in small_copies[:3] + volt_copies + small_copies[3:]:
        copy.start()

    barrier = pltpu.get_barrier_semaphore()

    def greet(hop):
        pl.semaphore_signal(
            barrier, inc=1, device_id=(group, lax.rem(me + hop, members)),
            device_id_type=MESH_ID,
        )

    def greet_some(i, _):
        for own in range(GROUPED):
            greet(1 + i * GROUPED + own)
        return 0

    lax.fori_loop(0, (members - 1) // GROUPED, greet_some, 0)
    for hop in range((members - 1) // GROUPED * GROUPED + 1, members):
        greet(hop)

    for copy in small_copies[:3]:
        copy.wait()
    rows = formed.shape[1]
    points, beams = table.shape[1], rows // 2
    select = lax.broadcasted_iota(jnp.int32, (points, beams), 0) == point_ref[...]
    double = (
        lax.broadcasted_iota(jnp.int32, (beams, rows), 1) // 2
        == lax.broadcasted_iota(jnp.int32, (beams, rows), 0)
    )
    select = jnp.dot(
        jnp.where(select, 1.0, 0.0).astype(jnp.bfloat16),
        jnp.where(double, 1.0, 0.0).astype(jnp.bfloat16),
        preferred_element_type=jnp.float32,
    )
    delay = jnp.dot(
        table[...], select, precision=HIGHEST, preferred_element_type=jnp.float32
    )
    delay = jnp.concatenate([delay, delay], 0).T
    dishes = delay.shape[1] // 2
    part_out = lax.broadcasted_iota(jnp.int32, delay.shape, 0) & 1
    part_in = (lax.broadcasted_iota(jnp.int32, delay.shape, 1) >= dishes).astype(jnp.int32)
    offset = 0.25 * (part_in - part_out).astype(jnp.float32)
    gain = mask_ref[...].astype(jnp.float32) * (1.0 / math.sqrt(dishes))
    gain = jnp.concatenate([gain, gain], 1)
    def turn(chans):
        return circle_turns((chans * BAND_WIDTH / CHANS) * delay)

    cosine, sine = circle_turns(freq_ref[0] * delay - offset)
    wave[0, 0] = cosine * gain
    wave[0, 1] = sine * gain
    step[0], step[1] = turn(chunks)
    for slot in range(1, chunk):
        wave[slot, 0], wave[slot, 1] = times(
            wave[slot - 1, 0], wave[slot - 1, 1], step[0], step[1]
        )
    step[0], step[1] = turn(LINES)
    for slot in range(chunk, slots):
        wave[slot, 0], wave[slot, 1] = times(
            wave[slot - chunk, 0], wave[slot - chunk, 1], step[0], step[1]
        )
    step[0], step[1] = turn(1)

    for c in range(chunks):
        volt_copies[c].wait()

        def form(slot, _, c=c):
            re_part = wave[slot, 0]
            im_part = wave[slot, 1]
            formed[c * slots + slot] = jnp.dot(
                re_part.astype(jnp.bfloat16), volt[slot, c], preferred_element_type=jnp.float32
            ).astype(jnp.bfloat16)
            wave[slot, 0], wave[slot, 1] = times(re_part, im_part, step[0], step[1])
            return 0

        lax.fori_loop(0, slots, form, 0)
        if c == 0:
            pl.semaphore_wait(barrier, members - 1)

        def send(to, c=c):
            here = pl.ds(c * slots, slots)
            pltpu.make_async_remote_copy(
                src_ref=formed.at[here, pl.ds(pl.multiple_of(2 * to, 2), 2)],
                dst_ref=landed.at[here, pl.ds(pl.multiple_of(2 * me, 2), 2)],
                send_sem=send_sem,
                recv_sem=recv_sems.at[c],
                device_id=(group, to),
                device_id_type=MESH_ID,
            ).start()

        def send_some(i, _, send=send):
            for own in range(GROUPED):
                place = lax.rem((1 + i * GROUPED + own) * SPREAD, chips)
                to_y = lax.rem(my_y + lax.div(place, rows_x), rows_y)
                to_x = lax.rem(my_x + lax.rem(place, rows_x), rows_x)
                chip = (to_y * rows_x + to_x) * cores
                for core in range(cores):
                    send(chip + core)
            return 0

        lax.fori_loop(0, (chips - 1) // GROUPED, send_some, 0)
        for other in range(1, cores):
            send(me - my_core + lax.rem(my_core + other, cores))

    small_copies[3].wait()
    tables(rate_ref[0], rate_ref[1], tw_ref, tm_ref, q_ref, em_ref, f_ref)

    total_ref[...] = jnp.zeros_like(total_ref)
    block = pl.ds(pl.multiple_of((me // 8) * 16, 16), 16)
    mine = lax.broadcasted_iota(jnp.int32, (slots, 16, formed.shape[2]), 1) // 2 == me % 8
    most = pl.ds(0, 2 * (members - 1))
    for c in range(chunks):
        here = pl.ds(c * slots, slots)
        pltpu.make_async_remote_copy(
            src_ref=formed.at[here, most],
            dst_ref=landed.at[here, most],
            send_sem=send_sem,
            recv_sem=recv_sems.at[c],
            device_id=(group, me),
            device_id_type=MESH_ID,
        ).wait_recv()
        landed[here, block, :] = jnp.where(
            mine, formed[here, block, :].astype(jnp.float32),
            landed[here, block, :].astype(jnp.float32),
        ).astype(jnp.bfloat16)
        for pair in range(chunk // 2):
            first = c * slots + 2 * pair
            data = jnp.concatenate(
                [
                    jnp.concatenate(
                        [landed[first + half * chunk], landed[first + half * chunk + 1]], 1
                    )
                    for half in range(2)
                ],
                0,
            )
            wide = data.astype(jnp.float32)
            total_ref[...] += jnp.sum((wide * wide).reshape(-1, 8, 2 * RADIX), 0)
            mixed = jnp.dot(am_ref[...], data, preferred_element_type=jnp.float32)
            grid_ref[c + 2 * pair * chunks] = mixed[:, :RADIX]
            grid_ref[c + (2 * pair + 1) * chunks] = mixed[:, RADIX:]

        def chan_fours(i, _, c=c):
            here = pl.ds(pl.multiple_of(i * 16, 16), 16)
            there = pl.ds(pl.multiple_of(i * 16 + 2 * RADIX, 16), 16)
            lines = [c + chunks * high for high in range(4)]
            values = [
                times(grid_ref[n, here], grid_ref[n, there], tw_ref[0, n, here], tw_ref[1, n, here])
                for n in lines
            ]
            for first, pair in enumerate(four(values, 1)):
                re_part, im_part = sixteenth(pair, c * first, 1)
                grid_ref[lines[first], here] = re_part
                grid_ref[lines[first], there] = im_part
            return 0

        lax.fori_loop(0, 2 * RADIX // 16, chan_fours, 0)
    pltpu.make_async_remote_copy(
        src_ref=formed.at[:, most],
        dst_ref=landed.at[:, most],
        send_sem=send_sem,
        recv_sem=recv_sems.at[0],
        device_id=(group, me),
        device_id_type=MESH_ID,
    ).wait_send()


def tables(rate, inverse, tw_ref, tm_ref, q_ref, em_ref, f_ref):
    piece = 32

    def position(shape, axis):
        return lax.broadcasted_iota(jnp.int32, shape, axis)

    shape = (piece, RADIX)
    per = 2 * RADIX // piece

    def chan_turn(i, _):
        line, start = i // per, pl.multiple_of((i % per) * piece, piece)
        row = position(shape, 0) + start
        low = row & (RADIX - 1)
        chan_unit = line * (2 * low + row // RADIX) * (LENGTH // CHANS)
        cosine, sine = circle_units(
            chan_unit + inverse * (position(shape, 1) * low) * (LENGTH // RADIX)
        )
        tw_ref[0, line, pl.ds(start, piece)] = cosine
        tw_ref[1, line, pl.ds(start, piece)] = sine
        return 0

    lax.fori_loop(0, LINES * per, chan_turn, 0)

    wide = (piece, 2 * RADIX)
    per_wide = RADIX // piece

    def time_matrix(i, _):
        start = pl.multiple_of(i * piece, piece)
        time = position(wide, 0) + start
        beat = position(wide, 1) // 2
        parity = position(wide, 1) & 1
        cosine, sine = circle_units(-inverse * (time * beat) * (LENGTH // RADIX))
        for own in range(2):
            keep = parity == own
            re_part = jnp.where(keep, cosine, 0.0)
            im_part = jnp.where(keep, sine, 0.0)
            from_re = pl.ds(start + 2 * own * RADIX, piece)
            from_im = pl.ds(start + (2 * own + 1) * RADIX, piece)
            tm_ref[from_re, : 2 * RADIX] = re_part.astype(jnp.bfloat16)
            tm_ref[from_re, 2 * RADIX :] = im_part.astype(jnp.bfloat16)
            tm_ref[from_im, : 2 * RADIX] = (-im_part).astype(jnp.bfloat16)
            tm_ref[from_im, 2 * RADIX :] = re_part.astype(jnp.bfloat16)
        return 0

    lax.fori_loop(0, per_wide, time_matrix, 0)

    def wide_turn(i, _):
        line, start = i // per_wide, pl.multiple_of((i % per_wide) * piece, piece)
        low = position(wide, 0) + start
        beat = position(wide, 1) // 2
        here = pl.ds(start, piece)
        cosine, sine = circle_units(
            inverse
            * (
                low * (low - 2 * beat)
                + line * line * (LENGTH // 32)
                + line * (low - beat) * (LENGTH // 2048)
            )
        )
        q_ref[0, line, here] = cosine
        q_ref[1, line, here] = sine
        cosine, sine = circle_units(
            inverse
            * (
                beat * (beat + line * (LENGTH // 2048) + low * (LENGTH // RADIX))
                + line * line * (LENGTH // 32)
            )
            - rate * (LENGTH // 8)
        )
        f_ref[0, line, here] = cosine
        f_ref[1, line, here] = sine
        return 0

    lax.fori_loop(0, LINES * per_wide, wide_turn, 0)

    def end_matrix(i, _):
        line, start = i // per_wide, pl.multiple_of((i % per_wide) * piece, piece)
        high = position(shape, 0) + start
        cosine, sine = circle_units(
            -inverse * (position(shape, 1) * (LINES * high + line)) * (LENGTH // 2048)
        )
        upper = pl.ds(start, piece)
        lower = pl.ds(start + RADIX, piece)
        em_ref[line, upper, :RADIX] = cosine.astype(jnp.bfloat16)
        em_ref[line, upper, RADIX:] = (-sine).astype(jnp.bfloat16)
        em_ref[line, lower, :RADIX] = sine.astype(jnp.bfloat16)
        em_ref[line, lower, RADIX:] = cosine.astype(jnp.bfloat16)
        return 0

    lax.fori_loop(0, LINES * per_wide, end_matrix, 0)


def chain_kernel(
    rate_ref, mixed_ref, total_ref, tw_ref, tm_ref, q_ref, em_ref, f_ref, out_ref,
    grid, mid, held, sems,
):
    def chan_lines(i, _):
        here = pl.ds(pl.multiple_of(i * 8, 8), 8)
        there = pl.ds(pl.multiple_of(i * 8 + 2 * RADIX, 8), 8)
        for first in range(4):
            column = [
                (mixed_ref[low + 4 * first, here], mixed_ref[low + 4 * first, there])
                for low in range(4)
            ]
            for second, (re_part, im_part) in enumerate(four(column, 1)):
                grid[first + 4 * second, here] = re_part
                grid[first + 4 * second, there] = im_part
        return 0

    lax.fori_loop(0, 2 * RADIX // 8, chan_lines, 0, unroll=2)

    for quad in range(LINES // 4):
        rows = []
        for n in range(4 * quad, 4 * quad + 4):
            parts = [
                grid[n, part * 2 * RADIX + own * RADIX : part * 2 * RADIX + (own + 1) * RADIX]
                for own in range(2)
                for part in range(2)
            ]
            rows.append(jnp.concatenate(parts, 1).astype(jnp.bfloat16))
        mixed = jnp.dot(
            jnp.concatenate(rows, 0), tm_ref[...], preferred_element_type=jnp.float32
        )
        for n in range(4):
            mid[4 * quad + n] = mixed[n * RADIX : (n + 1) * RADIX]

    def beat_lines(i, _):
        here = pl.ds(pl.multiple_of(i * 8, 8), 8)
        for lane in range(0, 2 * RADIX, RADIX):
            re_at = slice(lane, lane + RADIX)
            im_at = slice(lane + 2 * RADIX, lane + 3 * RADIX)
            values = [
                times(
                    mid[n, here, re_at], mid[n, here, im_at],
                    q_ref[0, n, here, re_at], q_ref[1, n, here, re_at],
                )
                for n in range(LINES)
            ]
            for n, (re_part, im_part) in enumerate(sixteen(values, -1)):
                mid[n, here, re_at] = re_part
                mid[n, here, im_at] = im_part
        return 0

    lax.fori_loop(0, RADIX // 8, beat_lines, 0, unroll=2)

    power = jnp.sum(jnp.sum(total_ref[...], 1, keepdims=True), 0, keepdims=True) * (1.0 / LENGTH)
    factor = lax.rsqrt(power + EPSILON) * (
        math.sqrt(2.0 / LENGTH) / math.sqrt(CHANS)
    )
    factor = jnp.broadcast_to(factor, (8, 2 * RADIX))[:1]
    copies = []
    for line in range(LINES):
        source = (rate_ref[1] * line) & (LINES - 1)
        data = jnp.concatenate(
            [mid[source, :, : 2 * RADIX], mid[source, :, 2 * RADIX :]], 0
        ).astype(jnp.bfloat16)
        mixed = jnp.dot(em_ref[line], data, preferred_element_type=jnp.float32)
        re_part, im_part = times(
            mixed[:RADIX], mixed[RADIX:], f_ref[0, line] * factor, f_ref[1, line] * factor
        )
        lanes = slice(line * 2 * RADIX, (line + 1) * 2 * RADIX)
        held[0, :, lanes] = re_part
        held[1, :, lanes] = im_part
        copy = pltpu.make_async_copy(
            held.at[:, :, pl.ds(line * 2 * RADIX, 2 * RADIX)],
            out_ref.at[0, :, :, pl.ds(line * 2 * RADIX, 2 * RADIX)],
            sems.at[line],
        )
        copy.start()
        copies.append(copy)
    for copy in copies:
        copy.wait()


def chan_matrix(members):
    n1 = np.arange(2 * RADIX)
    row_n1 = 2 * (n1 % RADIX) + n1 // RADIX
    half, member = np.meshgrid(np.arange(2), np.arange(members), indexing="ij")
    coarse = (2 * member + half).reshape(-1)
    angle = 2.0 * np.pi * ((row_n1[:, None] * coarse[None, :]) % (2 * RADIX)) / (2 * RADIX)
    cosine, sine = np.cos(angle), np.sin(angle)
    upper = np.stack([cosine, -sine], -1).reshape(2 * RADIX, -1)
    lower = np.stack([sine, cosine], -1).reshape(2 * RADIX, -1)
    return jnp.asarray(np.concatenate([upper, lower], 0), jnp.bfloat16)


def on_device(sizes, voltages, delays, pointing, dm_index, dish_mask):
    chan_dev, parts, dishes, samples = voltages.shape
    beams = pointing.shape[0]
    members = math.prod(sizes)
    rows = parts * beams
    first_chan = (lax.axis_index("chan") * chan_dev).astype(jnp.float32)
    frequency = (BAND_LOW + BAND_WIDTH * (first_chan + 0.5) / CHANS).reshape(1)
    rate = (2 * dm_index + 1).reshape(1)
    inverse = rate
    for _ in range(4):
        inverse = inverse * (2 - rate * inverse)
    rates = jnp.concatenate([rate, inverse & (LENGTH - 1)])
    wide = 2 * RADIX
    chunks = 4
    slots = chan_dev // chunks
    mixed, total, tw, tm, q, em, f = pl.pallas_call(
        functools.partial(front_kernel, sizes),
        out_shape=[
            jax.ShapeDtypeStruct((LINES, 2 * wide, samples), jnp.float32),
            jax.ShapeDtypeStruct((8, wide), jnp.float32),
            jax.ShapeDtypeStruct((2, LINES, wide, samples), jnp.float32),
            jax.ShapeDtypeStruct((2 * wide, 2 * wide), jnp.bfloat16),
            jax.ShapeDtypeStruct((2, LINES, RADIX, wide), jnp.float32),
            jax.ShapeDtypeStruct((LINES, wide, wide), jnp.bfloat16),
            jax.ShapeDtypeStruct((2, LINES, RADIX, wide), jnp.float32),
        ],
        in_specs=[SMEM_SPEC] * 2 + [HBM_SPEC] * 5,
        out_specs=[VMEM_SPEC] * 7,
        scratch_shapes=[
            pltpu.VMEM((slots, chunks, parts * dishes, samples), jnp.bfloat16),
            pltpu.VMEM(delays.shape[::-1], jnp.float32),
            pltpu.VMEM((1, beams), jnp.int32),
            pltpu.VMEM((1, dishes), jnp.int32),
            pltpu.VMEM((2 * wide, 2 * wide), jnp.bfloat16),
            pltpu.VMEM((slots, 2, rows, parts * dishes), jnp.float32),
            pltpu.VMEM((2, rows, parts * dishes), jnp.float32),
            pltpu.VMEM((chan_dev, rows, samples), jnp.bfloat16),
            pltpu.VMEM((chan_dev, rows, samples), jnp.bfloat16),
            pltpu.SemaphoreType.DMA((chunks,)),
            pltpu.SemaphoreType.DMA((4,)),
            pltpu.SemaphoreType.DMA(()),
            pltpu.SemaphoreType.DMA((chunks,)),
        ],
        compiler_params=pltpu.CompilerParams(
            collective_id=0, has_side_effects=True, vmem_limit_bytes=20 << 20
        ),
        name="front",
    )(
        rates,
        frequency,
        *(
            pltpu.with_memory_space_constraint(value, pltpu.HBM)
            for value in (
                pointing.reshape(1, beams),
                dish_mask.reshape(1, dishes),
                chan_matrix(members),
                voltages.reshape(slots, chunks, parts * dishes, samples),
                delays.T,
            )
        ),
    )
    return pl.pallas_call(
        chain_kernel,
        out_shape=jax.ShapeDtypeStruct((1, 2, samples, CHANS), jnp.float32),
        in_specs=[SMEM_SPEC] + [VMEM_SPEC] * 7,
        out_specs=ANY_SPEC,
        scratch_shapes=[
            pltpu.VMEM((LINES, 2 * wide, samples), jnp.float32),
            pltpu.VMEM((LINES, RADIX, 2 * wide), jnp.float32),
            pltpu.VMEM((2, samples, CHANS), jnp.float32),
            pltpu.SemaphoreType.DMA((LINES,)),
        ],
        compiler_params=pltpu.CompilerParams(vmem_limit_bytes=20 << 20),
        name="chain",
    )(rates, mixed, total, tw, tm, q, em, f)


def solution(mesh):
    members = mesh.shape["chan"]
    cores = 2
    side = math.isqrt(members // cores)
    sizes = (members // cores // side, side, cores)
    placed = (P(("grp", "chan")), P(), P("grp"), P(("grp", "chan")), P("grp"))
    return jax.shard_map(
        functools.partial(on_device, sizes),
        mesh=mesh,
        in_specs=placed,
        out_specs=P(("grp", "chan")),
        check_vma=False,
    )
```
